32 devices in a mesh: kpt: 4 (over z), row: 2 (over x), col: 4 (over y, core).
Axes of the slice: x: 2, y: 2, z: 4, core: 2. Of those that a mesh axis runs over, the one named last changes fastest.
Arguments:
- occ_orbitals: bfloat16 [4, 2048, 256], P('kpt', 'row'), may hold values from -6 to 6
- empty_orbitals: bfloat16 [4, 2048, 896], P('kpt', 'row'), may hold values from -6 to 6
- occ_energy: float32 [4, 256], replicated, may hold values from 0.05 to 2
- empty_energy: float32 [4, 896], replicated, may hold values from 0.05 to 2
- tau_points: float32 [3], replicated, may hold values from 0.3 to 3
- partner: int32 [4], replicated, may hold values from 0 to 3, each once
- mirror: int32 [2048], P('col'), may hold values from 0 to 2047, each once
Outputs:
- polarization: float32 [3, 2, 1024, 2048], P(None, 'row', 'kpt', 'col')
The draws below stay inside these ranges and needn't reach their ends.
Inputs may be any that keep to these rules, and one draw needn't show every extreme that they name: Each k-point is the partner of exactly one k-point. `mirror`: each grid point is the column of exactly one window column.
All inputs are finite; a program needn't handle non-finite values.
Results may differ from the reference program's by a relative error of at most 0.0003.
Values may be sent and summed in bfloat16 or wider, within the bound.
A program may use at most 64 MiB of HBM per device.

```python
import math
import jax
import jax.numpy as jnp
from jax import lax

NOCC = 256
NEMP = 896
TAUS = 3
ROW_DEV = 1024
KPOINTS = 4
GRID = 2048
COLS = 2048
ROW_BLOCKS = 2


def block_levels(own_key, dims, cuts, least, high):
    def one(dim, shards_of):
        draws = jax.random.uniform(jax.random.fold_in(jax.random.fold_in(own_key, 6), dim), (shards_of,), jnp.float32, least / len(cuts), high / len(cuts))
        return jnp.repeat(jnp.exp(draws), dims[dim] // shards_of).reshape((-1,) + (1,) * (len(dims) - dim - 1))

    gain = one(*cuts[0])
    for cut in cuts[1:]:
        gain = gain * one(*cut)
    return gain


def noise(stream_key, shape, scale, reach, shards=(), held_as=jnp.bfloat16):
    gain = block_levels(stream_key, shape, shards, -0.22, 0.18) if shards else 1.0
    array = jax.random.normal(stream_key, shape, jnp.float32) * scale * gain
    return jnp.minimum(jnp.maximum(array, -reach), reach).astype(held_as)


def setup_inputs(seed: int = 0) -> dict:
    key_of = jax.random.split(jax.random.key(seed), 8)
    return {
        "occ_orbitals": noise(key_of[0], (KPOINTS, GRID, NOCC), 1.0, 6.0, ((0, 4), (1, 2))),
        "empty_orbitals": noise(key_of[1], (KPOINTS, GRID, NEMP), 1.0, 6.0, ((0, 4), (1, 2))),
        "occ_energy": jnp.clip(jnp.exp(jax.random.uniform(key_of[2], (KPOINTS, NOCC), jnp.float32, math.log(0.05), math.log(2.0))), 0.05, 2.0),
        "empty_energy": jnp.clip(jnp.exp(jax.random.uniform(key_of[3], (KPOINTS, NEMP), jnp.float32, math.log(0.05), math.log(2.0))), 0.05, 2.0),
        "tau_points": jnp.clip(jnp.exp(jax.random.uniform(key_of[4], (TAUS,), jnp.float32, math.log(0.3), math.log(3.0))), 0.3, 3.0),
        "partner": jax.random.permutation(key_of[5], KPOINTS).astype(jnp.int32),
        "mirror": jax.random.permutation(key_of[6], GRID).astype(jnp.int32),
    }


def green_tile(rows, cols, weight, width):
    scaled = (rows.astype(jnp.float32) * weight[None, :]).astype(jnp.bfloat16)
    tile = lax.dot_general(scaled, cols, (((1,), (1,)), ((), ())), preferred_element_type=jnp.float32)
    return tile * (1.0 / math.sqrt(width))

def reference(occ_orbitals, empty_orbitals, occ_energy, empty_energy, tau_points, partner, mirror):

    def one_kpoint(kpoint, total):
        other = partner[kpoint]
        occ_rows = lax.dynamic_index_in_dim(occ_orbitals, kpoint, 0, keepdims=False)
        empty_rows = lax.dynamic_index_in_dim(empty_orbitals, other, 0, keepdims=False)
        occ_levels = lax.dynamic_index_in_dim(occ_energy, kpoint, 0, keepdims=False)
        empty_levels = lax.dynamic_index_in_dim(empty_energy, other, 0, keepdims=False)
        occ_cols = jnp.take(occ_rows, mirror, axis=0)
        empty_cols = jnp.take(empty_rows, mirror, axis=0)
        slabs = []
        for time_index in range(TAUS):
            occ_weight = jnp.exp(-tau_points[time_index] * occ_levels)
            empty_weight = jnp.exp(-tau_points[time_index] * empty_levels)
            occ_green = green_tile(occ_rows, occ_cols, occ_weight, NOCC)
            empty_green = green_tile(empty_rows, empty_cols, empty_weight, NEMP)
            slabs.append(occ_green * empty_green)
        return total + jnp.stack(slabs, axis=0)
    start = jnp.zeros((TAUS, GRID, COLS), jnp.float32)
    total = lax.fori_loop(0, KPOINTS, one_kpoint, start)
    total = total * (-1.0 / math.sqrt(KPOINTS))
    return total.reshape(TAUS, ROW_BLOCKS, ROW_DEV, COLS)
```

```python
import functools
import math

import jax
import jax.numpy as jnp
from jax import lax
from jax.experimental import pallas as pl
from jax.experimental.pallas import tpu as pltpu
from jax.sharding import PartitionSpec as P

NOCC = 256
NEMP = 896
TAUS = 3
LINE_BYTES = 40 * 2**20
CHUNKS = 4
LANES = 128
TILE = 16


def green_tile(rows, cols, weight, width):
    scaled = (rows.astype(jnp.float32) * weight[None, :]).astype(jnp.bfloat16)
    tile = lax.dot_general(
        scaled, cols, (((1,), (1,)), ((), ())), preferred_element_type=jnp.float32
    )
    return tile * (1.0 / math.sqrt(width))


def permute_block(block, source):
    spread = lax.all_to_all(block, "kpt", split_axis=1, concat_axis=0, tiled=True)
    arranged = jnp.take(spread, source, axis=0)
    return lax.all_to_all(arranged, "kpt", split_axis=0, concat_axis=1, tiled=True)


def shards_reduced(occ_orbitals, empty_orbitals, occ_energy, empty_energy, tau_points, partner, mirror):
    kpoints = lax.axis_size("kpt")
    own_index = lax.axis_index("kpt")
    kpoint_ids = jnp.arange(kpoints, dtype=jnp.int32)
    matches = partner[None, :] == kpoint_ids[:, None]
    inverse = jnp.sum(jnp.where(matches, kpoint_ids[None, :], 0), axis=1)
    occ_block = permute_block(occ_orbitals, inverse)
    occ_kpoint = inverse[own_index]
    occ_rows = occ_block[0]
    empty_rows = empty_orbitals[0]
    occ_levels = lax.dynamic_index_in_dim(occ_energy, occ_kpoint, 0, keepdims=False)
    empty_levels = lax.dynamic_index_in_dim(empty_energy, own_index, 0, keepdims=False)
    occ_full, empty_full = (
        lax.all_gather(occ_rows, "row", axis=0, tiled=True),
        lax.all_gather(empty_rows, "row", axis=0, tiled=True),
    )
    occ_cols = jnp.take(occ_full, mirror, axis=0)
    empty_cols = jnp.take(empty_full, mirror, axis=0)
    factor = -1.0 / math.sqrt(kpoints)
    slabs = []
    for time_index in range(TAUS):
        occ_weight = jnp.exp(-tau_points[time_index] * occ_levels)
        empty_weight = jnp.exp(-tau_points[time_index] * empty_levels)
        occ_green = green_tile(occ_rows, occ_cols, occ_weight, NOCC)
        empty_green = green_tile(empty_rows, empty_cols, empty_weight, NEMP)
        slabs.append(occ_green * empty_green * factor)
    product_term = jnp.stack(slabs, axis=0)[:, None, :, :]
    return lax.psum_scatter(product_term, "kpt", scatter_dimension=2, tiled=True)


def line_kernel(kpoints, columns, scale,
                tau_ref, partner_ref, mirror_ref, occ_energy_ref, empty_energy_ref, occ_ref, empty_ref, out_ref,
                cols, mine, pre_out, pre_in, rows_occ, rows_empty, scaled_occ, scaled_empty, green_occ, green_empty,
                send_p, recv_p, send_r, recv_r, send_f, recv_f,
                send_u, recv_u, send_d, recv_d, send_x, recv_x):
    me, own_row, own_col = lax.axis_index("kpt"), lax.axis_index("row"), lax.axis_index("col")
    nrows, nocc = occ_ref.shape
    width = nocc + empty_ref.shape[1]
    slab = nrows // kpoints
    part = slab // columns
    half = mine.shape[0]
    size = half // CHUNKS
    times = tau_ref.shape[0]
    last = kpoints - 1
    across = {"row": 1 - own_row}
    above, below = {"kpt": lax.rem(me + 1, kpoints)}, {"kpt": lax.rem(me + last, kpoints)}

    def remote(src, dst, send_sem, recv_sem, device):
        return pltpu.make_async_remote_copy(
            src_ref=src, dst_ref=dst, send_sem=send_sem, recv_sem=recv_sem,
            device_id=device, device_id_type=pl.DeviceIdType.MESH,
        )

    barrier = pltpu.get_barrier_semaphore()
    peers = [{"kpt": lax.rem(me + d, kpoints)} for d in range(1, kpoints)]
    peers += [across]
    peers += [{"col": lax.rem(own_col + e, columns)} for e in range(1, columns)]
    for peer in peers:
        pl.semaphore_signal(barrier, inc=1, device_id=peer, device_id_type=pl.DeviceIdType.MESH)
    pl.semaphore_wait(barrier, len(peers))

    def row_copies(d):
        other = lax.rem(me + d, kpoints)
        start = pl.multiple_of((other * columns + own_col) * part, part)
        return [
            remote(src.at[pl.ds(start, part), :], dst.at[me, own_col], send_r.at[i, d], recv_r.at[i, d], {"kpt": other})
            for i, (src, dst) in enumerate(((occ_ref, rows_occ), (empty_ref, rows_empty)))
        ]

    def row_forwards(d):
        source = lax.rem(me + kpoints - d, kpoints)
        return [
            remote(dst.at[source, own_col], dst.at[source, own_col], send_f.at[i, d, e], recv_f.at[i, d, e],
                   {"col": lax.rem(own_col + e, columns)})
            for e in range(1, columns)
            for i, dst in enumerate((rows_occ, rows_empty))
        ]

    def pre_copy(c):
        piece = pl.ds(c * size, size)
        return remote(pre_out.at[piece], pre_in.at[piece], send_p.at[c], recv_p.at[c], across)

    def cross_copy(k, c):
        piece = cols.at[k, own_row, pl.ds(c * size, size)]
        return remote(piece, piece, send_x.at[k, c], recv_x.at[k, c], across)

    def up_copy(s, c):
        piece = cols.at[lax.rem(me - s + kpoints, kpoints), own_row, pl.ds(c * size, size)]
        return remote(piece, piece, send_u.at[s, c], recv_u.at[s, c], above)

    def down_copy(s, c):
        piece = cols.at[lax.rem(me + s, kpoints), own_row, pl.ds(c * size, size)]
        return remote(piece, piece, send_d.at[s, c], recv_d.at[s, c], below)

    for d in range(1, kpoints):
        for copy in row_copies(d):
            copy.start()

    def pick(first):
        index = mirror_ref[0:1, pl.ds(pl.multiple_of(first, LANES), LANES)] - own_row * nrows
        index = jnp.transpose(jnp.broadcast_to(index, (LANES, LANES)))
        lane = lax.broadcasted_iota(jnp.int32, (LANES, LANES), 1)
        hot = jnp.concatenate(
            [jnp.where(index == lane + b, 1.0, 0.0).astype(jnp.bfloat16) for b in range(0, nrows, LANES)], axis=1)
        dot = functools.partial(jnp.dot, hot, preferred_element_type=jnp.float32)
        return dot(occ_ref[...]).astype(jnp.bfloat16), dot(empty_ref[...]).astype(jnp.bfloat16)

    def fill(dst, whose):
        for first in range(0, half, LANES):
            occ, empty = pick(whose * half + first)
            dst[first:first + LANES, :nocc] = occ
            dst[first:first + LANES, nocc:] = empty
            yield range(first // size, (first + LANES) // size)

    for chunks in fill(pre_out, 1 - own_row):
        for c in chunks:
            pre_copy(c).start()
    for _ in fill(mine, own_row):
        pass

    for c in range(columns):
        start = pl.multiple_of(me * slab + c * part, part)
        rows_occ[me, c] = occ_ref[pl.ds(start, part), :]
        rows_empty[me, c] = empty_ref[pl.ds(start, part), :]

    def scale_rows(k):
        for rows, energy, scaled in ((rows_occ, occ_energy_ref, scaled_occ), (rows_empty, empty_energy_ref, scaled_empty)):
            held = energy[...]
            pick_k = lax.broadcasted_iota(jnp.int32, held.shape, 0) == k
            levels = jnp.sum(jnp.where(pick_k, held, 0.0), axis=0, keepdims=True)
            weights = [jnp.exp(-tau_ref[t] * levels) for t in range(times)]

            @pl.loop(0, columns)
            def _(c):
                block = rows[k, c].astype(jnp.float32)
                for t in range(times):
                    start = pl.multiple_of(t * slab + c * part, part)
                    scaled[k, pl.ds(start, part), :] = (block * weights[t]).astype(jnp.bfloat16)

    def multiply(k, h):
        window = pl.ds(pl.multiple_of(h * half, half), half)

        @pl.loop(0, times)
        def _(t):
            rows = pl.ds(pl.multiple_of(t * slab, slab), slab)
            for scaled, green, lo, hi in ((scaled_occ, green_occ, 0, nocc), (scaled_empty, green_empty, nocc, width)):
                green[k, rows, window] = lax.dot_general(
                    scaled[k, rows, :], cols[k, h, :, lo:hi], (((1,), (1,)), ((), ())),
                    preferred_element_type=jnp.float32)

    def combine(h):
        window = pl.ds(pl.multiple_of(h * half, half), half)

        @pl.loop(0, times * slab, step=TILE)
        def _(start):
            rows = pl.ds(pl.multiple_of(start, TILE), TILE)
            total = green_occ[0, rows, window] * green_empty[partner_ref[0], rows, window]
            for k in range(1, kpoints):
                total += green_occ[k, rows, window] * green_empty[partner_ref[k], rows, window]
            out_ref[rows, window] = total * scale

    scale_rows(me)
    for c in range(CHUNKS):
        piece = pl.ds(c * size, size)
        pre_copy(c).wait_recv()
        cols[me, own_row, piece] = (mine[piece].astype(jnp.float32) + pre_in[piece].astype(jnp.float32)).astype(jnp.bfloat16)
        pl.when(me < last)(up_copy(0, c).start)
        pl.when(me > 0)(down_copy(0, c).start)
        cross_copy(me, c).start()
        if 0 < c < kpoints:
            for copy in row_copies(c):
                copy.wait_recv()
            for copy in row_forwards(c):
                copy.start()
    for d in range(CHUNKS, kpoints):
        for copy in row_copies(d):
            copy.wait_recv()
        for copy in row_forwards(d):
            copy.start()
    multiply(me, own_row)

    def partner_at(i):
        value, bit = me, 1
        while bit < kpoints:
            if i & bit:
                value = value + bit - 2 * bit * lax.rem(me // bit, 2)
            bit *= 2
        return value

    for s in range(last):
        for c in range(CHUNKS):
            @pl.when(me > s)
            def _():
                up_copy(s, c).wait_recv()
                pl.when(me < last)(up_copy(s + 1, c).start)
                cross_copy(lax.rem(me - 1 - s + kpoints, kpoints), c).start()

            @pl.when(me < last - s)
            def _():
                down_copy(s, c).wait_recv()
                pl.when(me > 0)(down_copy(s + 1, c).start)
                cross_copy(lax.rem(me + 1 + s, kpoints), c).start()
        if s == 0:
            for d in range(1, kpoints):
                for copy in row_forwards(d):
                    copy.wait_recv()
        source = partner_at(s + 1)
        scale_rows(source)
        multiply(source, own_row)
    combine(own_row)
    for i in range(kpoints):
        source = partner_at(i)
        for c in range(CHUNKS):
            cross_copy(source, c).wait_recv()
        multiply(source, 1 - own_row)
    combine(1 - own_row)

    for d in range(1, kpoints):
        for copy in row_copies(d) + row_forwards(d):
            copy.wait_send()
    for c in range(CHUNKS):
        pre_copy(c).wait_send()
        for k in range(kpoints):
            cross_copy(k, c).wait_send()
        for s in range(last):
            pl.when((me < last) & (me >= s))(up_copy(s, c).wait_send)
            pl.when((me > 0) & (me + s <= last))(down_copy(s, c).wait_send)


def line(occ, empty, occ_energy, empty_energy, tau_points, partner, mirror, kpoints, columns, scale):
    nrows, nocc = occ.shape
    nemp = empty.shape[1]
    width = nocc + nemp
    window, times = mirror.shape[0], tau_points.shape[0]
    half, slab = window // 2, nrows // kpoints
    part = slab // columns
    dma = pltpu.SemaphoreType.DMA
    vmem = pl.BlockSpec(memory_space=pltpu.VMEM)
    smem = pl.BlockSpec(memory_space=pltpu.SMEM)
    bf16, f32 = jnp.bfloat16, jnp.float32
    return pl.pallas_call(
        functools.partial(line_kernel, kpoints, columns, scale),
        out_shape=jax.ShapeDtypeStruct((times * slab, window), f32),
        in_specs=[smem, smem, vmem, vmem, vmem, vmem, vmem],
        out_specs=vmem,
        scratch_shapes=[
            pltpu.VMEM((kpoints, 2, half, width), bf16),
            pltpu.VMEM((half, width), bf16),
            pltpu.VMEM((half, width), bf16),
            pltpu.VMEM((half, width), bf16),
            pltpu.VMEM((kpoints, columns, part, nocc), bf16),
            pltpu.VMEM((kpoints, columns, part, nemp), bf16),
            pltpu.VMEM((kpoints, times * slab, nocc), bf16),
            pltpu.VMEM((kpoints, times * slab, nemp), bf16),
            pltpu.VMEM((kpoints, times * slab, window), f32),
            pltpu.VMEM((kpoints, times * slab, window), f32),
            dma((CHUNKS,)), dma((CHUNKS,)),
            dma((2, kpoints)), dma((2, kpoints)),
            dma((2, kpoints, columns)), dma((2, kpoints, columns)),
            dma((kpoints, CHUNKS)), dma((kpoints, CHUNKS)),
            dma((kpoints, CHUNKS)), dma((kpoints, CHUNKS)),
            dma((kpoints, CHUNKS)), dma((kpoints, CHUNKS)),
        ],
        compiler_params=pltpu.CompilerParams(collective_id=0, has_side_effects=True),
        name="line",
    )(tau_points, partner, mirror.reshape(1, window), occ_energy, empty_energy, occ, empty)


def shards_line(occ_orbitals, empty_orbitals, occ_energy, empty_energy, tau_points, partner, mirror):
    kpoints, columns = lax.axis_size("kpt"), lax.axis_size("col")
    scale = -1.0 / math.sqrt(kpoints) / math.sqrt(NOCC) / math.sqrt(NEMP)
    total = line(
        occ_orbitals[0], empty_orbitals[0], occ_energy, empty_energy, tau_points, partner, mirror,
        kpoints, columns, scale)
    return total.reshape(tau_points.shape[0], 1, -1, mirror.shape[0])


def shards(*args):
    kpoints, columns = lax.axis_size("kpt"), lax.axis_size("col")
    nrows, nocc, nemp = args[0].shape[1], args[0].shape[2], args[1].shape[2]
    times, window = args[4].shape[0], args[6].shape[0]
    slab, width = nrows // kpoints, nocc + nemp
    held = 2 * width * (kpoints * window + 4 * nrows + times * nrows) + 8 * times * nrows * window
    aligned = window % (2 * LANES) == 0 and nrows % LANES == 0 and nocc % LANES == 0 and nemp % LANES == 0
    aligned = aligned and (slab // columns) % 16 == 0 and slab % columns == 0 and nrows % kpoints == 0
    fits = aligned and held <= LINE_BYTES and kpoints & (kpoints - 1) == 0
    if lax.axis_size("row") == 2 and fits:
        return shards_line(*args)
    return shards_reduced(*args)


def solution(mesh):
    return jax.shard_map(
        shards,
        mesh=mesh,
        in_specs=(P("kpt", "row", None), P("kpt", "row", None), P(), P(), P(), P(), P("col")),
        out_specs=P(None, "row", "kpt", "col"),
        check_vma=False,
    )
```

```python
import functools
import math

import jax
import jax.numpy as jnp
from jax import lax
from jax.experimental import pallas as pl
from jax.experimental.pallas import tpu as pltpu
from jax.sharding import PartitionSpec as P

NOCC = 256
NEMP = 896
TAUS = 3
LINE_BYTES = 40 * 2**20
KERNEL_BYTES = 60 * 1024 * 2**10
CHUNKS = 4
EXTRAS = (1, 1, 0)
LANES = 128
TILE = 16


def green_tile(rows, cols, weight, width):
    scaled = (rows.astype(jnp.float32) * weight[None, :]).astype(jnp.bfloat16)
    tile = lax.dot_general(
        scaled, cols, (((1,), (1,)), ((), ())), preferred_element_type=jnp.float32
    )
    return tile * (1.0 / math.sqrt(width))


def permute_block(block, source):
    spread = lax.all_to_all(block, "kpt", split_axis=1, concat_axis=0, tiled=True)
    arranged = jnp.take(spread, source, axis=0)
    return lax.all_to_all(arranged, "kpt", split_axis=0, concat_axis=1, tiled=True)


def shards_reduced(occ_orbitals, empty_orbitals, occ_energy, empty_energy, tau_points, partner, mirror):
    kpoints = lax.axis_size("kpt")
    own_index = lax.axis_index("kpt")
    kpoint_ids = jnp.arange(kpoints, dtype=jnp.int32)
    matches = partner[None, :] == kpoint_ids[:, None]
    inverse = jnp.sum(jnp.where(matches, kpoint_ids[None, :], 0), axis=1)
    occ_block = permute_block(occ_orbitals, inverse)
    occ_kpoint = inverse[own_index]
    occ_rows = occ_block[0]
    empty_rows = empty_orbitals[0]
    occ_levels = lax.dynamic_index_in_dim(occ_energy, occ_kpoint, 0, keepdims=False)
    empty_levels = lax.dynamic_index_in_dim(empty_energy, own_index, 0, keepdims=False)
    occ_full, empty_full = (
        lax.all_gather(occ_rows, "row", axis=0, tiled=True),
        lax.all_gather(empty_rows, "row", axis=0, tiled=True),
    )
    occ_cols = jnp.take(occ_full, mirror, axis=0)
    empty_cols = jnp.take(empty_full, mirror, axis=0)
    factor = -1.0 / math.sqrt(kpoints)
    slabs = []
    for time_index in range(TAUS):
        occ_weight = jnp.exp(-tau_points[time_index] * occ_levels)
        empty_weight = jnp.exp(-tau_points[time_index] * empty_levels)
        occ_green = green_tile(occ_rows, occ_cols, occ_weight, NOCC)
        empty_green = green_tile(empty_rows, empty_cols, empty_weight, NEMP)
        slabs.append(occ_green * empty_green * factor)
    product_term = jnp.stack(slabs, axis=0)[:, None, :, :]
    return lax.psum_scatter(product_term, "kpt", scatter_dimension=2, tiled=True)


def line_kernel(kpoints, columns, scale,
                tau_in, partner_in, mirror_in, occ_energy_in, empty_energy_in, occ_in, empty_in, out_ref,
                tau_ref, partner_ref, mirror_ref, occ_energy_ref, empty_energy_ref, occ_ref, empty_ref, local_sem,
                cols, mine, pre_out, pre_in, rows_occ, rows_empty, scaled_occ, scaled_empty, green_occ, green_empty,
                send_p, recv_p, send_r, recv_r, send_f, recv_f,
                send_u, recv_u, send_d, recv_d, send_x, recv_x, send_y, recv_y, send_z, recv_z):
    me, own_row, own_col = lax.axis_index("kpt"), lax.axis_index("row"), lax.axis_index("col")
    nrows, nocc = occ_ref.shape
    width = nocc + empty_ref.shape[1]
    slab = nrows // kpoints
    part = slab // columns
    half = mine.shape[0]
    size = half // CHUNKS
    times = tau_ref.shape[0]
    last = kpoints - 1
    across = {"row": 1 - own_row}
    above, below = {"kpt": lax.rem(me + 1, kpoints)}, {"kpt": lax.rem(me + last, kpoints)}

    def remote(src, dst, send_sem, recv_sem, device):
        return pltpu.make_async_remote_copy(
            src_ref=src, dst_ref=dst, send_sem=send_sem, recv_sem=recv_sem,
            device_id=device, device_id_type=pl.DeviceIdType.MESH,
        )

    loads = [
        pltpu.make_async_copy(src, dst, local_sem.at[i])
        for i, (src, dst) in enumerate((
            (mirror_in, mirror_ref), (occ_in, occ_ref), (empty_in, empty_ref), (occ_energy_in, occ_energy_ref),
            (empty_energy_in, empty_energy_ref), (tau_in, tau_ref), (partner_in, partner_ref)))
    ]
    for copy in loads:
        copy.start()
    barrier = pltpu.get_barrier_semaphore()
    peers = [{"kpt": lax.rem(me + d, kpoints)} for d in range(1, kpoints)]
    peers += [across]
    peers += [{"col": lax.rem(own_col + e, columns)} for e in range(1, columns)]
    for peer in peers:
        pl.semaphore_signal(barrier, inc=1, device_id=peer, device_id_type=pl.DeviceIdType.MESH)
    for copy in loads:
        copy.wait()
    pl.semaphore_wait(barrier, len(peers))

    def row_copies(d):
        other = lax.rem(me + d, kpoints)
        start = pl.multiple_of((other * columns + own_col) * part, part)
        return [
            remote(src.at[pl.ds(start, part), :], dst.at[me, own_col], send_r.at[i, d], recv_r.at[i, d], {"kpt": other})
            for i, (src, dst) in enumerate(((occ_ref, rows_occ), (empty_ref, rows_empty)))
        ]

    def row_forwards(d):
        source = lax.rem(me + kpoints - d, kpoints)
        return [
            remote(dst.at[source, own_col], dst.at[source, own_col], send_f.at[i, d, e], recv_f.at[i, d, e],
                   {"col": lax.rem(own_col + e, columns)})
            for e in range(1, columns)
            for i, dst in enumerate((rows_occ, rows_empty))
        ]

    def pre_copy(c):
        piece = pl.ds(c * size, size)
        return remote(pre_out.at[piece], pre_in.at[piece], send_p.at[c], recv_p.at[c], across)

    def cross_copy(k, c):
        piece = cols.at[k, own_row, pl.ds(c * size, size)]
        return remote(piece, piece, send_x.at[k, c], recv_x.at[k, c], across)

    def up_copy(s, c):
        piece = cols.at[lax.rem(me - s + kpoints, kpoints), own_row, pl.ds(c * size, size)]
        return remote(piece, piece, send_u.at[s, c], recv_u.at[s, c], above)

    def down_copy(s, c):
        piece = cols.at[lax.rem(me + s, kpoints), own_row, pl.ds(c * size, size)]
        return remote(piece, piece, send_d.at[s, c], recv_d.at[s, c], below)

    def extras(s):
        return EXTRAS[min(s, len(EXTRAS) - 1)] if s < last else 0

    def extra_up(s, c):
        piece = cols.at[lax.rem(me - s + kpoints, kpoints), 1 - own_row, pl.ds(c * size, size)]
        return remote(piece, piece, send_y.at[s, c], recv_y.at[s, c], above)

    def extra_down(s, c):
        piece = cols.at[lax.rem(me + s, kpoints), 1 - own_row, pl.ds(c * size, size)]
        return remote(piece, piece, send_z.at[s, c], recv_z.at[s, c], below)

    def pass_extras(s):
        for c in range(extras(s)):
            @pl.when(me > s)
            def _():
                extra_up(s, c).wait_recv()
                if c < extras(s + 1):
                    pl.when(me < last)(extra_up(s + 1, c).start)

            @pl.when(me < last - s)
            def _():
                extra_down(s, c).wait_recv()
                if c < extras(s + 1):
                    pl.when(me > 0)(extra_down(s + 1, c).start)

    for d in range(1, kpoints):
        for copy in row_copies(d):
            copy.start()

    def pick(first):
        index = mirror_ref[0:1, pl.ds(pl.multiple_of(first, LANES), LANES)] - own_row * nrows
        index = jnp.transpose(jnp.broadcast_to(index, (LANES, LANES)))
        lane = lax.broadcasted_iota(jnp.int32, (LANES, LANES), 1)
        hot = jnp.concatenate(
            [jnp.where(index == lane + b, 1.0, 0.0).astype(jnp.bfloat16) for b in range(0, nrows, LANES)], axis=1)
        dot = functools.partial(jnp.dot, hot, preferred_element_type=jnp.float32)
        return dot(occ_ref[...]).astype(jnp.bfloat16), dot(empty_ref[...]).astype(jnp.bfloat16)

    def fill(dst, whose):
        for first in range(0, half, LANES):
            occ, empty = pick(whose * half + first)
            dst[first:first + LANES, :nocc] = occ
            dst[first:first + LANES, nocc:] = empty
            yield range(first // size, (first + LANES) // size)

    for chunks in fill(pre_out, 1 - own_row):
        for c in chunks:
            pre_copy(c).start()
    for _ in fill(mine, own_row):
        pass

    for c in range(columns):
        start = pl.multiple_of(me * slab + c * part, part)
        rows_occ[me, c] = occ_ref[pl.ds(start, part), :]
        rows_empty[me, c] = empty_ref[pl.ds(start, part), :]

    def scale_rows(k):
        for rows, energy, scaled in ((rows_occ, occ_energy_ref, scaled_occ), (rows_empty, empty_energy_ref, scaled_empty)):
            held = energy[...]
            pick_k = lax.broadcasted_iota(jnp.int32, held.shape, 0) == k
            levels = jnp.sum(jnp.where(pick_k, held, 0.0), axis=0, keepdims=True)
            weights = [jnp.exp(-tau_ref[t] * levels) for t in range(times)]

            @pl.loop(0, columns)
            def _(c):
                block = rows[k, c].astype(jnp.float32)
                for t in range(times):
                    start = pl.multiple_of(t * slab + c * part, part)
                    scaled[k, pl.ds(start, part), :] = (block * weights[t]).astype(jnp.bfloat16)

    def multiply(k, h):
        window = pl.ds(pl.multiple_of(h * half, half), half)

        @pl.loop(0, times)
        def _(t):
            rows = pl.ds(pl.multiple_of(t * slab, slab), slab)
            for scaled, green, lo, hi in ((scaled_occ, green_occ, 0, nocc), (scaled_empty, green_empty, nocc, width)):
                green[k, rows, window] = lax.dot_general(
                    scaled[k, rows, :], cols[k, h, :, lo:hi], (((1,), (1,)), ((), ())),
                    preferred_element_type=jnp.float32)

    def combine(h):
        window = pl.ds(pl.multiple_of(h * half, half), half)

        @pl.loop(0, times * slab, step=TILE)
        def _(start):
            rows = pl.ds(pl.multiple_of(start, TILE), TILE)
            total = green_occ[0, rows, window] * green_empty[partner_ref[0], rows, window]
            for k in range(1, kpoints):
                total += green_occ[k, rows, window] * green_empty[partner_ref[k], rows, window]
            out_ref[rows, window] = total * scale

    scale_rows(me)
    for c in range(CHUNKS):
        piece = pl.ds(c * size, size)
        pre_copy(c).wait_recv()
        cols[me, own_row, piece] = (mine[piece].astype(jnp.float32) + pre_in[piece].astype(jnp.float32)).astype(jnp.bfloat16)
        pl.when(me < last)(up_copy(0, c).start)
        pl.when(me > 0)(down_copy(0, c).start)
        cross_copy(me, c).start()
        if 0 < c < kpoints:
            for copy in row_copies(c):
                copy.wait_recv()
            for copy in row_forwards(c):
                copy.start()
    for d in range(CHUNKS, kpoints):
        for copy in row_copies(d):
            copy.wait_recv()
        for copy in row_forwards(d):
            copy.start()
    multiply(me, own_row)

    def partner_at(i):
        value, bit = me, 1
        while bit < kpoints:
            if i & bit:
                value = value + bit - 2 * bit * lax.rem(me // bit, 2)
            bit *= 2
        return value

    for s in range(last):
        for c in range(CHUNKS):
            @pl.when(me > s)
            def _():
                up_copy(s, c).wait_recv()
                pl.when(me < last)(up_copy(s + 1, c).start)
                if c >= extras(s):
                    cross_copy(lax.rem(me - 1 - s + kpoints, kpoints), c).start()

            @pl.when(me < last - s)
            def _():
                down_copy(s, c).wait_recv()
                pl.when(me > 0)(down_copy(s + 1, c).start)
                if c >= extras(s):
                    cross_copy(lax.rem(me + 1 + s, kpoints), c).start()
        if s == 0:
            for d in range(1, kpoints):
                for copy in row_forwards(d):
                    copy.wait_recv()
        source = partner_at(s + 1)
        scale_rows(source)
        multiply(source, own_row)
        if s == 0:
            for c in range(CHUNKS):
                cross_copy(me, c).wait_recv()
                if c < extras(0):
                    pl.when(me < last)(extra_up(0, c).start)
                    pl.when(me > 0)(extra_down(0, c).start)
            multiply(me, 1 - own_row)
        else:
            pass_extras(s - 1)
    combine(own_row)
    pass_extras(last - 1)
    for s in range(last):
        for c in range(extras(s), CHUNKS):
            @pl.when(me > s)
            def _():
                cross_copy(lax.rem(me - 1 - s + kpoints, kpoints), c).wait_recv()

            @pl.when(me < last - s)
            def _():
                cross_copy(lax.rem(me + 1 + s, kpoints), c).wait_recv()
        multiply(partner_at(s + 1), 1 - own_row)
    combine(1 - own_row)

    for d in range(1, kpoints):
        for copy in row_copies(d) + row_forwards(d):
            copy.wait_send()
    for c in range(CHUNKS):
        pre_copy(c).wait_send()
        cross_copy(me, c).wait_send()
        for s in range(last):
            if c >= extras(s):
                pl.when(me > s)(cross_copy(lax.rem(me - 1 - s + kpoints, kpoints), c).wait_send)
                pl.when(me < last - s)(cross_copy(lax.rem(me + 1 + s, kpoints), c).wait_send)
            else:
                pl.when((me < last) & (me >= s))(extra_up(s, c).wait_send)
                pl.when((me > 0) & (me + s <= last))(extra_down(s, c).wait_send)
            pl.when((me < last) & (me >= s))(up_copy(s, c).wait_send)
            pl.when((me > 0) & (me + s <= last))(down_copy(s, c).wait_send)


def line(occ, empty, occ_energy, empty_energy, tau_points, partner, mirror, kpoints, columns, scale):
    nrows, nocc = occ.shape
    nemp = empty.shape[1]
    width = nocc + nemp
    window, times = mirror.shape[0], tau_points.shape[0]
    half, slab = window // 2, nrows // kpoints
    part = slab // columns
    dma = pltpu.SemaphoreType.DMA
    hbm = pl.BlockSpec(memory_space=pltpu.HBM)
    bf16, f32 = jnp.bfloat16, jnp.float32
    return pl.pallas_call(
        functools.partial(line_kernel, kpoints, columns, scale),
        out_shape=jax.ShapeDtypeStruct((times * slab, window), f32),
        in_specs=[hbm] * 7,
        out_specs=pl.BlockSpec(memory_space=pltpu.VMEM),
        scratch_shapes=[
            pltpu.SMEM((times,), f32),
            pltpu.SMEM((kpoints,), jnp.int32),
            pltpu.VMEM((1, window), jnp.int32),
            pltpu.VMEM(occ_energy.shape, f32),
            pltpu.VMEM(empty_energy.shape, f32),
            pltpu.VMEM(occ.shape, bf16),
            pltpu.VMEM(empty.shape, bf16),
            dma((7,)),
            pltpu.VMEM((kpoints, 2, half, width), bf16),
            pltpu.VMEM((half, width), bf16),
            pltpu.VMEM((half, width), bf16),
            pltpu.VMEM((half, width), bf16),
            pltpu.VMEM((kpoints, columns, part, nocc), bf16),
            pltpu.VMEM((kpoints, columns, part, nemp), bf16),
            pltpu.VMEM((kpoints, times * slab, nocc), bf16),
            pltpu.VMEM((kpoints, times * slab, nemp), bf16),
            pltpu.VMEM((kpoints, times * slab, window), f32),
            pltpu.VMEM((kpoints, times * slab, window), f32),
            dma((CHUNKS,)), dma((CHUNKS,)),
            dma((2, kpoints)), dma((2, kpoints)),
            dma((2, kpoints, columns)), dma((2, kpoints, columns)),
            dma((kpoints, CHUNKS)), dma((kpoints, CHUNKS)),
            dma((kpoints, CHUNKS)), dma((kpoints, CHUNKS)),
            dma((kpoints, CHUNKS)), dma((kpoints, CHUNKS)),
            dma((kpoints, CHUNKS)), dma((kpoints, CHUNKS)),
            dma((kpoints, CHUNKS)), dma((kpoints, CHUNKS)),
        ],
        compiler_params=pltpu.CompilerParams(collective_id=0, has_side_effects=True, vmem_limit_bytes=KERNEL_BYTES),
        name="line",
    )(tau_points, partner, mirror.reshape(1, window), occ_energy, empty_energy, occ, empty)


def shards_line(occ_orbitals, empty_orbitals, occ_energy, empty_energy, tau_points, partner, mirror):
    kpoints, columns = lax.axis_size("kpt"), lax.axis_size("col")
    scale = -1.0 / math.sqrt(kpoints) / math.sqrt(NOCC) / math.sqrt(NEMP)
    total = line(
        occ_orbitals[0], empty_orbitals[0], occ_energy, empty_energy, tau_points, partner, mirror,
        kpoints, columns, scale)
    return total.reshape(tau_points.shape[0], 1, -1, mirror.shape[0])


def shards(*args):
    kpoints, columns = lax.axis_size("kpt"), lax.axis_size("col")
    nrows, nocc, nemp = args[0].shape[1], args[0].shape[2], args[1].shape[2]
    times, window = args[4].shape[0], args[6].shape[0]
    slab, width = nrows // kpoints, nocc + nemp
    held = 2 * width * (kpoints * window + 4 * nrows + times * nrows) + 8 * times * nrows * window
    aligned = window % (2 * LANES) == 0 and nrows % LANES == 0 and nocc % LANES == 0 and nemp % LANES == 0
    aligned = aligned and (slab // columns) % 16 == 0 and slab % columns == 0 and nrows % kpoints == 0
    fits = aligned and held <= LINE_BYTES and kpoints & (kpoints - 1) == 0
    if lax.axis_size("row") == 2 and fits:
        return shards_line(*args)
    return shards_reduced(*args)


def solution(mesh):
    return jax.shard_map(
        shards,
        mesh=mesh,
        in_specs=(P("kpt", "row", None), P("kpt", "row", None), P(), P(), P(), P(), P("col")),
        out_specs=P(None, "row", "kpt", "col"),
        check_vma=False,
    )
```

```python
import functools
import math

import jax
import jax.numpy as jnp
from jax import lax
from jax.experimental import pallas as pl
from jax.experimental.pallas import tpu as pltpu
from jax.sharding import PartitionSpec as P

NOCC = 256
NEMP = 896
TAUS = 3
LINE_BYTES = 40 * 2**20
KERNEL_BYTES = 48 * 2**20
CHUNKS = 4
EXTRAS = (1, 1, 0)
LANES = 128
TILE = 16


def green_tile(rows, cols, weight, width):
    scaled = (rows.astype(jnp.float32) * weight[None, :]).astype(jnp.bfloat16)
    tile = lax.dot_general(
        scaled, cols, (((1,), (1,)), ((), ())), preferred_element_type=jnp.float32
    )
    return tile * (1.0 / math.sqrt(width))


def permute_block(block, source):
    spread = lax.all_to_all(block, "kpt", split_axis=1, concat_axis=0, tiled=True)
    arranged = jnp.take(spread, source, axis=0)
    return lax.all_to_all(arranged, "kpt", split_axis=0, concat_axis=1, tiled=True)


def shards_reduced(occ_orbitals, empty_orbitals, occ_energy, empty_energy, tau_points, partner, mirror):
    kpoints = lax.axis_size("kpt")
    own_index = lax.axis_index("kpt")
    kpoint_ids = jnp.arange(kpoints, dtype=jnp.int32)
    matches = partner[None, :] == kpoint_ids[:, None]
    inverse = jnp.sum(jnp.where(matches, kpoint_ids[None, :], 0), axis=1)
    occ_block = permute_block(occ_orbitals, inverse)
    occ_kpoint = inverse[own_index]
    occ_rows = occ_block[0]
    empty_rows = empty_orbitals[0]
    occ_levels = lax.dynamic_index_in_dim(occ_energy, occ_kpoint, 0, keepdims=False)
    empty_levels = lax.dynamic_index_in_dim(empty_energy, own_index, 0, keepdims=False)
    occ_full, empty_full = (
        lax.all_gather(occ_rows, "row", axis=0, tiled=True),
        lax.all_gather(empty_rows, "row", axis=0, tiled=True),
    )
    occ_cols = jnp.take(occ_full, mirror, axis=0)
    empty_cols = jnp.take(empty_full, mirror, axis=0)
    factor = -1.0 / math.sqrt(kpoints)
    slabs = []
    for time_index in range(TAUS):
        occ_weight = jnp.exp(-tau_points[time_index] * occ_levels)
        empty_weight = jnp.exp(-tau_points[time_index] * empty_levels)
        occ_green = green_tile(occ_rows, occ_cols, occ_weight, NOCC)
        empty_green = green_tile(empty_rows, empty_cols, empty_weight, NEMP)
        slabs.append(occ_green * empty_green * factor)
    product_term = jnp.stack(slabs, axis=0)[:, None, :, :]
    return lax.psum_scatter(product_term, "kpt", scatter_dimension=2, tiled=True)


def line_kernel(kpoints, columns, scale,
                tau_in, partner_in, mirror_in, occ_energy_in, empty_energy_in, occ_in, empty_in, out_ref,
                tau_ref, partner_ref, mirror_ref, occ_energy_ref, empty_energy_ref, occ_ref, empty_ref, local_sem,
                cols, mine, pre_out, pre_in, rows_occ, rows_empty, scaled_occ, scaled_empty, green_occ, green_empty,
                send_p, recv_p, send_r, recv_r, send_f, recv_f,
                send_u, recv_u, send_d, recv_d, send_x, recv_x, send_y, recv_y, send_z, recv_z):
    me, own_row, own_col = lax.axis_index("kpt"), lax.axis_index("row"), lax.axis_index("col")
    nrows, nocc = occ_ref.shape
    width = nocc + empty_ref.shape[1]
    slab = nrows // kpoints
    part = slab // columns
    half = mine.shape[0]
    size = half // CHUNKS
    times = tau_ref.shape[0]
    last = kpoints - 1
    across = {"row": 1 - own_row}
    above, below = {"kpt": lax.rem(me + 1, kpoints)}, {"kpt": lax.rem(me + last, kpoints)}

    def remote(src, dst, send_sem, recv_sem, device):
        return pltpu.make_async_remote_copy(
            src_ref=src, dst_ref=dst, send_sem=send_sem, recv_sem=recv_sem,
            device_id=device, device_id_type=pl.DeviceIdType.MESH,
        )

    loads = [
        pltpu.make_async_copy(src, dst, local_sem.at[i])
        for i, (src, dst) in enumerate((
            (mirror_in, mirror_ref), (occ_in, occ_ref), (empty_in, empty_ref), (occ_energy_in, occ_energy_ref),
            (empty_energy_in, empty_energy_ref), (tau_in, tau_ref), (partner_in, partner_ref)))
    ]
    for copy in loads:
        copy.start()
    barrier = pltpu.get_barrier_semaphore()
    peers = [{"kpt": lax.rem(me + d, kpoints)} for d in range(1, kpoints)]
    peers += [across]
    peers += [{"col": lax.rem(own_col + e, columns)} for e in range(1, columns)]
    for peer in peers:
        pl.semaphore_signal(barrier, inc=1, device_id=peer, device_id_type=pl.DeviceIdType.MESH)
    for copy in loads:
        copy.wait()

    def row_copies(d):
        other = lax.rem(me + d, kpoints)
        start = pl.multiple_of((other * columns + own_col) * part, part)
        return [
            remote(src.at[pl.ds(start, part), :], dst.at[me, own_col], send_r.at[i, d], recv_r.at[i, d], {"kpt": other})
            for i, (src, dst) in enumerate(((occ_ref, rows_occ), (empty_ref, rows_empty)))
        ]

    def row_forwards(d):
        source = lax.rem(me + kpoints - d, kpoints)
        return [
            remote(dst.at[source, own_col], dst.at[source, own_col], send_f.at[i, d, e], recv_f.at[i, d, e],
                   {"col": lax.rem(own_col + e, columns)})
            for e in range(1, columns)
            for i, dst in enumerate((rows_occ, rows_empty))
        ]

    def pre_copy(c):
        piece = pl.ds(c * size, size)
        return remote(pre_out.at[piece], pre_in.at[piece], send_p.at[c], recv_p.at[c], across)

    def cross_copy(k, c):
        piece = cols.at[k, own_row, pl.ds(c * size, size)]
        return remote(piece, piece, send_x.at[k, c], recv_x.at[k, c], across)

    def up_copy(s, c):
        piece = cols.at[lax.rem(me - s + kpoints, kpoints), own_row, pl.ds(c * size, size)]
        return remote(piece, piece, send_u.at[s, c], recv_u.at[s, c], above)

    def down_copy(s, c):
        piece = cols.at[lax.rem(me + s, kpoints), own_row, pl.ds(c * size, size)]
        return remote(piece, piece, send_d.at[s, c], recv_d.at[s, c], below)

    def extras(s):
        return EXTRAS[min(s, len(EXTRAS) - 1)] if s < last else 0

    def extra_up(s, c):
        piece = cols.at[lax.rem(me - s + kpoints, kpoints), 1 - own_row, pl.ds(c * size, size)]
        return remote(piece, piece, send_y.at[s, c], recv_y.at[s, c], above)

    def extra_down(s, c):
        piece = cols.at[lax.rem(me + s, kpoints), 1 - own_row, pl.ds(c * size, size)]
        return remote(piece, piece, send_z.at[s, c], recv_z.at[s, c], below)

    def pass_extras(s):
        for c in range(extras(s)):
            @pl.when(me > s)
            def _():
                extra_up(s, c).wait_recv()
                if c < extras(s + 1):
                    pl.when(me < last)(extra_up(s + 1, c).start)

            @pl.when(me < last - s)
            def _():
                extra_down(s, c).wait_recv()
                if c < extras(s + 1):
                    pl.when(me > 0)(extra_down(s + 1, c).start)


    def pick(first):
        index = mirror_ref[0:1, pl.ds(pl.multiple_of(first, LANES), LANES)] - own_row * nrows
        index = jnp.transpose(jnp.broadcast_to(index, (LANES, LANES)))
        lane = lax.broadcasted_iota(jnp.int32, (LANES, LANES), 1)
        hot = jnp.concatenate(
            [jnp.where(index == lane + b, 1.0, 0.0).astype(jnp.bfloat16) for b in range(0, nrows, LANES)], axis=1)
        dot = functools.partial(jnp.dot, hot, preferred_element_type=jnp.float32)
        return dot(occ_ref[...]).astype(jnp.bfloat16), dot(empty_ref[...]).astype(jnp.bfloat16)

    def fill(dst, whose):
        for first in range(0, half, LANES):
            occ, empty = pick(whose * half + first)
            dst[first:first + LANES, :nocc] = occ
            dst[first:first + LANES, nocc:] = empty
            yield range(first // size, (first + LANES) // size)

    filling = fill(pre_out, 1 - own_row)
    ready = next(filling)
    pl.semaphore_wait(barrier, len(peers))
    for c in ready:
        pre_copy(c).start()
    for d in range(1, kpoints):
        for copy in row_copies(d):
            copy.start()
    for chunks in filling:
        for c in chunks:
            pre_copy(c).start()
    for _ in fill(mine, own_row):
        pass

    for c in range(columns):
        start = pl.multiple_of(me * slab + c * part, part)
        rows_occ[me, c] = occ_ref[pl.ds(start, part), :]
        rows_empty[me, c] = empty_ref[pl.ds(start, part), :]

    def scale_rows(k):
        for rows, energy, scaled in ((rows_occ, occ_energy_ref, scaled_occ), (rows_empty, empty_energy_ref, scaled_empty)):
            held = energy[...]
            pick_k = lax.broadcasted_iota(jnp.int32, held.shape, 0) == k
            levels = jnp.sum(jnp.where(pick_k, held, 0.0), axis=0, keepdims=True)
            weights = [jnp.exp(-tau_ref[t] * levels) for t in range(times)]

            @pl.loop(0, columns)
            def _(c):
                block = rows[k, c].astype(jnp.float32)
                for t in range(times):
                    start = pl.multiple_of(t * slab + c * part, part)
                    scaled[k, pl.ds(start, part), :] = (block * weights[t]).astype(jnp.bfloat16)

    def multiply(k, h):
        window = pl.ds(pl.multiple_of(h * half, half), half)

        @pl.loop(0, times)
        def _(t):
            rows = pl.ds(pl.multiple_of(t * slab, slab), slab)
            for scaled, green, lo, hi in ((scaled_occ, green_occ, 0, nocc), (scaled_empty, green_empty, nocc, width)):
                green[k, rows, window] = lax.dot_general(
                    scaled[k, rows, :], cols[k, h, :, lo:hi], (((1,), (1,)), ((), ())),
                    preferred_element_type=jnp.float32)

    def combine(h):
        window = pl.ds(pl.multiple_of(h * half, half), half)

        @pl.loop(0, times * slab, step=TILE)
        def _(start):
            rows = pl.ds(pl.multiple_of(start, TILE), TILE)
            total = green_occ[0, rows, window] * green_empty[partner_ref[0], rows, window]
            for k in range(1, kpoints):
                total += green_occ[k, rows, window] * green_empty[partner_ref[k], rows, window]
            out_ref[rows, window] = total * scale

    scale_rows(me)
    for c in range(CHUNKS):
        piece = pl.ds(c * size, size)
        pre_copy(c).wait_recv()
        cols[me, own_row, piece] = (mine[piece].astype(jnp.float32) + pre_in[piece].astype(jnp.float32)).astype(jnp.bfloat16)
        pl.when(me < last)(up_copy(0, c).start)
        pl.when(me > 0)(down_copy(0, c).start)
        cross_copy(me, c).start()
        if 0 < c < kpoints:
            for copy in row_copies(c):
                copy.wait_recv()
            for copy in row_forwards(c):
                copy.start()
    for d in range(CHUNKS, kpoints):
        for copy in row_copies(d):
            copy.wait_recv()
        for copy in row_forwards(d):
            copy.start()
    multiply(me, own_row)

    def partner_at(i):
        value, bit = me, 1
        while bit < kpoints:
            if i & bit:
                value = value + bit - 2 * bit * lax.rem(me // bit, 2)
            bit *= 2
        return value

    for s in range(last):
        for c in range(CHUNKS):
            @pl.when(me > s)
            def _():
                up_copy(s, c).wait_recv()
                pl.when(me < last)(up_copy(s + 1, c).start)
                if c >= extras(s):
                    cross_copy(lax.rem(me - 1 - s + kpoints, kpoints), c).start()

            @pl.when(me < last - s)
            def _():
                down_copy(s, c).wait_recv()
                pl.when(me > 0)(down_copy(s + 1, c).start)
                if c >= extras(s):
                    cross_copy(lax.rem(me + 1 + s, kpoints), c).start()
        if s == 0:
            for d in range(1, kpoints):
                for copy in row_forwards(d):
                    copy.wait_recv()
        source = partner_at(s + 1)
        scale_rows(source)
        multiply(source, own_row)
        if s == 0:
            for c in range(CHUNKS):
                cross_copy(me, c).wait_recv()
                if c < extras(0):
                    pl.when(me < last)(extra_up(0, c).start)
                    pl.when(me > 0)(extra_down(0, c).start)
            multiply(me, 1 - own_row)
        else:
            pass_extras(s - 1)
    combine(own_row)
    pass_extras(last - 1)
    for s in range(last):
        for c in range(extras(s), CHUNKS):
            @pl.when(me > s)
            def _():
                cross_copy(lax.rem(me - 1 - s + kpoints, kpoints), c).wait_recv()

            @pl.when(me < last - s)
            def _():
                cross_copy(lax.rem(me + 1 + s, kpoints), c).wait_recv()
        multiply(partner_at(s + 1), 1 - own_row)
    combine(1 - own_row)

    for d in range(1, kpoints):
        for copy in row_copies(d) + row_forwards(d):
            copy.wait_send()
    for c in range(CHUNKS):
        pre_copy(c).wait_send()
        cross_copy(me, c).wait_send()
        for s in range(last):
            if c >= extras(s):
                pl.when(me > s)(cross_copy(lax.rem(me - 1 - s + kpoints, kpoints), c).wait_send)
                pl.when(me < last - s)(cross_copy(lax.rem(me + 1 + s, kpoints), c).wait_send)
            else:
                pl.when((me < last) & (me >= s))(extra_up(s, c).wait_send)
                pl.when((me > 0) & (me + s <= last))(extra_down(s, c).wait_send)
            pl.when((me < last) & (me >= s))(up_copy(s, c).wait_send)
            pl.when((me > 0) & (me + s <= last))(down_copy(s, c).wait_send)


def line(occ, empty, occ_energy, empty_energy, tau_points, partner, mirror, kpoints, columns, scale):
    nrows, nocc = occ.shape
    nemp = empty.shape[1]
    width = nocc + nemp
    window, times = mirror.shape[0], tau_points.shape[0]
    half, slab = window // 2, nrows // kpoints
    part = slab // columns
    dma = pltpu.SemaphoreType.DMA
    hbm = pl.BlockSpec(memory_space=pltpu.HBM)
    bf16, f32 = jnp.bfloat16, jnp.float32
    return pl.pallas_call(
        functools.partial(line_kernel, kpoints, columns, scale),
        out_shape=jax.ShapeDtypeStruct((times * slab, window), f32),
        in_specs=[hbm] * 7,
        out_specs=pl.BlockSpec(memory_space=pltpu.VMEM),
        scratch_shapes=[
            pltpu.SMEM((times,), f32),
            pltpu.SMEM((kpoints,), jnp.int32),
            pltpu.VMEM((1, window), jnp.int32),
            pltpu.VMEM(occ_energy.shape, f32),
            pltpu.VMEM(empty_energy.shape, f32),
            pltpu.VMEM(occ.shape, bf16),
            pltpu.VMEM(empty.shape, bf16),
            dma((7,)),
            pltpu.VMEM((kpoints, 2, half, width), bf16),
            pltpu.VMEM((half, width), bf16),
            pltpu.VMEM((half, width), bf16),
            pltpu.VMEM((half, width), bf16),
            pltpu.VMEM((kpoints, columns, part, nocc), bf16),
            pltpu.VMEM((kpoints, columns, part, nemp), bf16),
            pltpu.VMEM((kpoints, times * slab, nocc), bf16),
            pltpu.VMEM((kpoints, times * slab, nemp), bf16),
            pltpu.VMEM((kpoints, times * slab, window), f32),
            pltpu.VMEM((kpoints, times * slab, window), f32),
            dma((CHUNKS,)), dma((CHUNKS,)),
            dma((2, kpoints)), dma((2, kpoints)),
            dma((2, kpoints, columns)), dma((2, kpoints, columns)),
            dma((kpoints, CHUNKS)), dma((kpoints, CHUNKS)),
            dma((kpoints, CHUNKS)), dma((kpoints, CHUNKS)),
            dma((kpoints, CHUNKS)), dma((kpoints, CHUNKS)),
            dma((kpoints, CHUNKS)), dma((kpoints, CHUNKS)),
            dma((kpoints, CHUNKS)), dma((kpoints, CHUNKS)),
        ],
        compiler_params=pltpu.CompilerParams(collective_id=0, has_side_effects=True, vmem_limit_bytes=KERNEL_BYTES),
        name="line",
    )(*(
        pltpu.with_memory_space_constraint(operand, pltpu.HBM)
        for operand in (tau_points, partner, mirror.reshape(1, window), occ_energy, empty_energy, occ, empty)
    ))


def shards_line(occ_orbitals, empty_orbitals, occ_energy, empty_energy, tau_points, partner, mirror):
    kpoints, columns = lax.axis_size("kpt"), lax.axis_size("col")
    scale = -1.0 / math.sqrt(kpoints) / math.sqrt(NOCC) / math.sqrt(NEMP)
    total = line(
        occ_orbitals[0], empty_orbitals[0], occ_energy, empty_energy, tau_points, partner, mirror,
        kpoints, columns, scale)
    return total.reshape(tau_points.shape[0], 1, -1, mirror.shape[0])


def shards(*args):
    kpoints, columns = lax.axis_size("kpt"), lax.axis_size("col")
    nrows, nocc, nemp = args[0].shape[1], args[0].shape[2], args[1].shape[2]
    times, window = args[4].shape[0], args[6].shape[0]
    slab, width = nrows // kpoints, nocc + nemp
    held = 2 * width * (kpoints * window + 4 * nrows + times * nrows) + 8 * times * nrows * window
    aligned = window % (2 * LANES) == 0 and nrows % LANES == 0 and nocc % LANES == 0 and nemp % LANES == 0
    aligned = aligned and (slab // columns) % 16 == 0 and slab % columns == 0 and nrows % kpoints == 0
    fits = aligned and held <= LINE_BYTES and kpoints & (kpoints - 1) == 0
    if lax.axis_size("row") == 2 and fits:
        return shards_line(*args)
    return shards_reduced(*args)


def solution(mesh):
    return jax.shard_map(
        shards,
        mesh=mesh,
        in_specs=(P("kpt", "row", None), P("kpt", "row", None), P(), P(), P(), P(), P("col")),
        out_specs=P(None, "row", "kpt", "col"),
        check_vma=False,
    )
```

```python
import functools
import math

import jax
import jax.numpy as jnp
from jax import lax
from jax.experimental import pallas as pl
from jax.experimental.pallas import tpu as pltpu
from jax.sharding import PartitionSpec as P

NOCC = 256
NEMP = 896
TAUS = 3
LINE_BYTES = 40 * 2**20
KERNEL_BYTES = 48 * 2**20
CHUNKS = 4
EXTRAS = (1, 1, 0)
LANES = 128
TILE = 16


def green_tile(rows, cols, weight, width):
    scaled = (rows.astype(jnp.float32) * weight[None, :]).astype(jnp.bfloat16)
    tile = lax.dot_general(
        scaled, cols, (((1,), (1,)), ((), ())), preferred_element_type=jnp.float32
    )
    return tile * (1.0 / math.sqrt(width))


def permute_block(block, source):
    spread = lax.all_to_all(block, "kpt", split_axis=1, concat_axis=0, tiled=True)
    arranged = jnp.take(spread, source, axis=0)
    return lax.all_to_all(arranged, "kpt", split_axis=0, concat_axis=1, tiled=True)


def shards_reduced(occ_orbitals, empty_orbitals, occ_energy, empty_energy, tau_points, partner, mirror):
    kpoints = lax.axis_size("kpt")
    own_index = lax.axis_index("kpt")
    kpoint_ids = jnp.arange(kpoints, dtype=jnp.int32)
    matches = partner[None, :] == kpoint_ids[:, None]
    inverse = jnp.sum(jnp.where(matches, kpoint_ids[None, :], 0), axis=1)
    occ_block = permute_block(occ_orbitals, inverse)
    occ_kpoint = inverse[own_index]
    occ_rows = occ_block[0]
    empty_rows = empty_orbitals[0]
    occ_levels = lax.dynamic_index_in_dim(occ_energy, occ_kpoint, 0, keepdims=False)
    empty_levels = lax.dynamic_index_in_dim(empty_energy, own_index, 0, keepdims=False)
    occ_full, empty_full = (
        lax.all_gather(occ_rows, "row", axis=0, tiled=True),
        lax.all_gather(empty_rows, "row", axis=0, tiled=True),
    )
    occ_cols = jnp.take(occ_full, mirror, axis=0)
    empty_cols = jnp.take(empty_full, mirror, axis=0)
    factor = -1.0 / math.sqrt(kpoints)
    slabs = []
    for time_index in range(TAUS):
        occ_weight = jnp.exp(-tau_points[time_index] * occ_levels)
        empty_weight = jnp.exp(-tau_points[time_index] * empty_levels)
        occ_green = green_tile(occ_rows, occ_cols, occ_weight, NOCC)
        empty_green = green_tile(empty_rows, empty_cols, empty_weight, NEMP)
        slabs.append(occ_green * empty_green * factor)
    product_term = jnp.stack(slabs, axis=0)[:, None, :, :]
    return lax.psum_scatter(product_term, "kpt", scatter_dimension=2, tiled=True)


def line_kernel(kpoints, columns, scale,
                tau_in, partner_in, mirror_in, occ_energy_in, empty_energy_in, occ_in, empty_in, out_ref,
                tau_ref, partner_ref, mirror_ref, occ_energy_ref, empty_energy_ref, occ_ref, empty_ref, local_sem,
                cols, mine, pre_out, pre_in, rows_occ, rows_empty, scaled_occ, scaled_empty, green_occ, green_empty,
                send_p, recv_p, send_r, recv_r, send_f, recv_f,
                send_u, recv_u, send_d, recv_d, send_x, recv_x, send_y, recv_y, send_z, recv_z):
    me, own_row, own_col = lax.axis_index("kpt"), lax.axis_index("row"), lax.axis_index("col")
    nrows, nocc = occ_ref.shape
    width = nocc + empty_ref.shape[1]
    slab = nrows // kpoints
    part = slab // columns
    half = mine.shape[0]
    size = half // CHUNKS
    times = tau_ref.shape[0]
    last = kpoints - 1
    across = {"row": 1 - own_row}
    above, below = {"kpt": lax.rem(me + 1, kpoints)}, {"kpt": lax.rem(me + last, kpoints)}

    def remote(src, dst, send_sem, recv_sem, device):
        return pltpu.make_async_remote_copy(
            src_ref=src, dst_ref=dst, send_sem=send_sem, recv_sem=recv_sem,
            device_id=device, device_id_type=pl.DeviceIdType.MESH,
        )

    loads = [
        pltpu.make_async_copy(src, dst, local_sem.at[i])
        for i, (src, dst) in enumerate((
            (mirror_in, mirror_ref), (occ_in, occ_ref), (empty_in, empty_ref), (occ_energy_in, occ_energy_ref),
            (empty_energy_in, empty_energy_ref), (tau_in, tau_ref), (partner_in, partner_ref)))
    ]
    for copy in loads:
        copy.start()
    barrier = pltpu.get_barrier_semaphore()
    peers = [{"kpt": lax.rem(me + d, kpoints)} for d in range(1, kpoints)]
    peers += [across]
    peers += [{"col": lax.rem(own_col + e, columns)} for e in range(1, columns)]
    for peer in peers:
        pl.semaphore_signal(barrier, inc=1, device_id=peer, device_id_type=pl.DeviceIdType.MESH)
    for copy in loads:
        copy.wait()

    def row_copies(d):
        other = lax.rem(me + d, kpoints)
        start = pl.multiple_of((other * columns + own_col) * part, part)
        return [
            remote(src.at[pl.ds(start, part), :], dst.at[me, own_col], send_r.at[i, d], recv_r.at[i, d], {"kpt": other})
            for i, (src, dst) in enumerate(((occ_ref, rows_occ), (empty_ref, rows_empty)))
        ]

    def row_forwards(d):
        source = lax.rem(me + kpoints - d, kpoints)
        return [
            remote(dst.at[source, own_col], dst.at[source, own_col], send_f.at[i, d, e], recv_f.at[i, d, e],
                   {"col": lax.rem(own_col + e, columns)})
            for e in range(1, columns)
            for i, dst in enumerate((rows_occ, rows_empty))
        ]

    def pre_copy(c):
        piece = pl.ds(c * size, size)
        return remote(pre_out.at[piece], pre_in.at[piece], send_p.at[c], recv_p.at[c], across)

    def cross_copy(k, c):
        piece = cols.at[k, own_row, pl.ds(c * size, size)]
        return remote(piece, piece, send_x.at[k, c], recv_x.at[k, c], across)

    def own_cross(g):
        piece = cols.at[me, own_row, pl.ds(g * 2 * size, 2 * size)]
        return remote(piece, piece, send_x.at[me, g], recv_x.at[me, g], across)

    def up_copy(s, c):
        piece = cols.at[lax.rem(me - s + kpoints, kpoints), own_row, pl.ds(c * size, size)]
        return remote(piece, piece, send_u.at[s, c], recv_u.at[s, c], above)

    def down_copy(s, c):
        piece = cols.at[lax.rem(me + s, kpoints), own_row, pl.ds(c * size, size)]
        return remote(piece, piece, send_d.at[s, c], recv_d.at[s, c], below)

    def extras(s):
        return EXTRAS[min(s, len(EXTRAS) - 1)] if s < last else 0

    def extra_up(s, c):
        piece = cols.at[lax.rem(me - s + kpoints, kpoints), 1 - own_row, pl.ds(c * size, size)]
        return remote(piece, piece, send_y.at[s, c], recv_y.at[s, c], above)

    def extra_down(s, c):
        piece = cols.at[lax.rem(me + s, kpoints), 1 - own_row, pl.ds(c * size, size)]
        return remote(piece, piece, send_z.at[s, c], recv_z.at[s, c], below)

    def pass_extras(s):
        for c in range(extras(s)):
            @pl.when(me > s)
            def _():
                extra_up(s, c).wait_recv()
                if c < extras(s + 1):
                    pl.when(me < last)(extra_up(s + 1, c).start)

            @pl.when(me < last - s)
            def _():
                extra_down(s, c).wait_recv()
                if c < extras(s + 1):
                    pl.when(me > 0)(extra_down(s + 1, c).start)


    def pick(first):
        index = mirror_ref[0:1, pl.ds(pl.multiple_of(first, LANES), LANES)] - own_row * nrows
        index = jnp.transpose(jnp.broadcast_to(index, (LANES, LANES)))
        lane = lax.broadcasted_iota(jnp.int32, (LANES, LANES), 1)
        hot = jnp.concatenate(
            [jnp.where(index == lane + b, 1.0, 0.0).astype(jnp.bfloat16) for b in range(0, nrows, LANES)], axis=1)
        dot = functools.partial(jnp.dot, hot, preferred_element_type=jnp.float32)
        return dot(occ_ref[...]).astype(jnp.bfloat16), dot(empty_ref[...]).astype(jnp.bfloat16)

    def fill(dst, whose):
        for first in range(0, half, LANES):
            occ, empty = pick(whose * half + first)
            dst[first:first + LANES, :nocc] = occ
            dst[first:first + LANES, nocc:] = empty
            yield range(first // size, (first + LANES) // size)

    filling = fill(pre_out, 1 - own_row)
    ready = next(filling)
    pl.semaphore_wait(barrier, len(peers))
    for c in ready:
        pre_copy(c).start()
    for d in range(1, kpoints):
        for copy in row_copies(d):
            copy.start()
    for chunks in filling:
        for c in chunks:
            pre_copy(c).start()
    for _ in fill(mine, own_row):
        pass

    for c in range(columns):
        start = pl.multiple_of(me * slab + c * part, part)
        rows_occ[me, c] = occ_ref[pl.ds(start, part), :]
        rows_empty[me, c] = empty_ref[pl.ds(start, part), :]

    def scale_rows(k):
        for rows, energy, scaled in ((rows_occ, occ_energy_ref, scaled_occ), (rows_empty, empty_energy_ref, scaled_empty)):
            held = energy[...]
            pick_k = lax.broadcasted_iota(jnp.int32, held.shape, 0) == k
            levels = jnp.sum(jnp.where(pick_k, held, 0.0), axis=0, keepdims=True)
            weights = [jnp.exp(-tau_ref[t] * levels) for t in range(times)]

            @pl.loop(0, columns)
            def _(c):
                block = rows[k, c].astype(jnp.float32)
                for t in range(times):
                    start = pl.multiple_of(t * slab + c * part, part)
                    scaled[k, pl.ds(start, part), :] = (block * weights[t]).astype(jnp.bfloat16)

    def multiply(k, h, lo_slot=0, slots=half):
        window = pl.ds(pl.multiple_of(h * half + lo_slot, slots), slots)

        @pl.loop(0, times)
        def _(t):
            rows = pl.ds(pl.multiple_of(t * slab, slab), slab)
            for scaled, green, lo, hi in ((scaled_occ, green_occ, 0, nocc), (scaled_empty, green_empty, nocc, width)):
                green[k, rows, window] = lax.dot_general(
                    scaled[k, rows, :], cols[k, h, lo_slot:lo_slot + slots, lo:hi], (((1,), (1,)), ((), ())),
                    preferred_element_type=jnp.float32)

    def combine(h, lo_slot=0, slots=half):
        window = pl.ds(pl.multiple_of(h * half + lo_slot, slots), slots)

        @pl.loop(0, times * slab, step=TILE)
        def _(start):
            rows = pl.ds(pl.multiple_of(start, TILE), TILE)
            total = green_occ[0, rows, window] * green_empty[partner_ref[0], rows, window]
            for k in range(1, kpoints):
                total += green_occ[k, rows, window] * green_empty[partner_ref[k], rows, window]
            out_ref[rows, window] = total * scale

    scale_rows(me)
    for c in range(CHUNKS):
        piece = pl.ds(c * size, size)
        pre_copy(c).wait_recv()
        cols[me, own_row, piece] = (mine[piece].astype(jnp.float32) + pre_in[piece].astype(jnp.float32)).astype(jnp.bfloat16)
        pl.when(me < last)(up_copy(0, c).start)
        pl.when(me > 0)(down_copy(0, c).start)
        if c % 2:
            own_cross(c // 2).start()
        if 0 < c < kpoints:
            for copy in row_copies(c):
                copy.wait_recv()
            for copy in row_forwards(c):
                copy.start()
    for d in range(CHUNKS, kpoints):
        for copy in row_copies(d):
            copy.wait_recv()
        for copy in row_forwards(d):
            copy.start()
    multiply(me, own_row)

    def partner_at(i):
        value, bit = me, 1
        while bit < kpoints:
            if i & bit:
                value = value + bit - 2 * bit * lax.rem(me // bit, 2)
            bit *= 2
        return value

    for s in range(last):
        for c in range(CHUNKS):
            @pl.when(me > s)
            def _():
                up_copy(s, c).wait_recv()
                pl.when(me < last)(up_copy(s + 1, c).start)
                if c >= extras(s):
                    cross_copy(lax.rem(me - 1 - s + kpoints, kpoints), c).start()

            @pl.when(me < last - s)
            def _():
                down_copy(s, c).wait_recv()
                pl.when(me > 0)(down_copy(s + 1, c).start)
                if c >= extras(s):
                    cross_copy(lax.rem(me + 1 + s, kpoints), c).start()
        if s == 0:
            for d in range(1, kpoints):
                for copy in row_forwards(d):
                    copy.wait_recv()
        if s == min(1, last - 1):
            if s == 0:
                for g in range(CHUNKS // 2):
                    own_cross(g).wait_recv()
            for c in range(extras(0)):
                pl.when(me < last)(extra_up(0, c).start)
                pl.when(me > 0)(extra_down(0, c).start)
        source = partner_at(s + 1)
        scale_rows(source)
        multiply(source, own_row)
        if s == 0:
            if last > 1:
                for g in range(CHUNKS // 2):
                    own_cross(g).wait_recv()
            multiply(me, 1 - own_row)
        if s > 1:
            pass_extras(s - 2)
    combine(own_row)
    for s in range(max(last - 2, 0), last):
        pass_extras(s)
    def take_crossed(s, chunks):
        for c in chunks:
            @pl.when(me > s)
            def _():
                cross_copy(lax.rem(me - 1 - s + kpoints, kpoints), c).wait_recv()

            @pl.when(me < last - s)
            def _():
                cross_copy(lax.rem(me + 1 + s, kpoints), c).wait_recv()

    for s in range(last - 1):
        take_crossed(s, range(extras(s), CHUNKS))
        multiply(partner_at(s + 1), 1 - own_row)
    for first in range(0, half, LANES):
        take_crossed(last - 1, range(max(extras(last - 1), first // size), (first + LANES) // size))
        multiply(partner_at(last), 1 - own_row, first, LANES)
        combine(1 - own_row, first, LANES)

    for d in range(1, kpoints):
        for copy in row_copies(d) + row_forwards(d):
            copy.wait_send()
    for c in range(CHUNKS):
        pre_copy(c).wait_send()
        if c % 2:
            own_cross(c // 2).wait_send()
        for s in range(last):
            if c >= extras(s):
                pl.when(me > s)(cross_copy(lax.rem(me - 1 - s + kpoints, kpoints), c).wait_send)
                pl.when(me < last - s)(cross_copy(lax.rem(me + 1 + s, kpoints), c).wait_send)
            else:
                pl.when((me < last) & (me >= s))(extra_up(s, c).wait_send)
                pl.when((me > 0) & (me + s <= last))(extra_down(s, c).wait_send)
            pl.when((me < last) & (me >= s))(up_copy(s, c).wait_send)
            pl.when((me > 0) & (me + s <= last))(down_copy(s, c).wait_send)


def line(occ, empty, occ_energy, empty_energy, tau_points, partner, mirror, kpoints, columns, scale):
    nrows, nocc = occ.shape
    nemp = empty.shape[1]
    width = nocc + nemp
    window, times = mirror.shape[0], tau_points.shape[0]
    half, slab = window // 2, nrows // kpoints
    part = slab // columns
    dma = pltpu.SemaphoreType.DMA
    hbm = pl.BlockSpec(memory_space=pltpu.HBM)
    bf16, f32 = jnp.bfloat16, jnp.float32
    return pl.pallas_call(
        functools.partial(line_kernel, kpoints, columns, scale),
        out_shape=jax.ShapeDtypeStruct((times * slab, window), f32),
        in_specs=[hbm] * 7,
        out_specs=pl.BlockSpec(memory_space=pltpu.VMEM),
        scratch_shapes=[
            pltpu.SMEM((times,), f32),
            pltpu.SMEM((kpoints,), jnp.int32),
            pltpu.VMEM((1, window), jnp.int32),
            pltpu.VMEM(occ_energy.shape, f32),
            pltpu.VMEM(empty_energy.shape, f32),
            pltpu.VMEM(occ.shape, bf16),
            pltpu.VMEM(empty.shape, bf16),
            dma((7,)),
            pltpu.VMEM((kpoints, 2, half, width), bf16),
            pltpu.VMEM((half, width), bf16),
            pltpu.VMEM((half, width), bf16),
            pltpu.VMEM((half, width), bf16),
            pltpu.VMEM((kpoints, columns, part, nocc), bf16),
            pltpu.VMEM((kpoints, columns, part, nemp), bf16),
            pltpu.VMEM((kpoints, times * slab, nocc), bf16),
            pltpu.VMEM((kpoints, times * slab, nemp), bf16),
            pltpu.VMEM((kpoints, times * slab, window), f32),
            pltpu.VMEM((kpoints, times * slab, window), f32),
            dma((CHUNKS,)), dma((CHUNKS,)),
            dma((2, kpoints)), dma((2, kpoints)),
            dma((2, kpoints, columns)), dma((2, kpoints, columns)),
            dma((kpoints, CHUNKS)), dma((kpoints, CHUNKS)),
            dma((kpoints, CHUNKS)), dma((kpoints, CHUNKS)),
            dma((kpoints, CHUNKS)), dma((kpoints, CHUNKS)),
            dma((kpoints, CHUNKS)), dma((kpoints, CHUNKS)),
            dma((kpoints, CHUNKS)), dma((kpoints, CHUNKS)),
        ],
        compiler_params=pltpu.CompilerParams(collective_id=0, has_side_effects=True, vmem_limit_bytes=KERNEL_BYTES),
        name="line",
    )(*(
        pltpu.with_memory_space_constraint(operand, pltpu.HBM)
        for operand in (tau_points, partner, mirror.reshape(1, window), occ_energy, empty_energy, occ, empty)
    ))


def shards_line(occ_orbitals, empty_orbitals, occ_energy, empty_energy, tau_points, partner, mirror):
    kpoints, columns = lax.axis_size("kpt"), lax.axis_size("col")
    scale = -1.0 / math.sqrt(kpoints) / math.sqrt(NOCC) / math.sqrt(NEMP)
    total = line(
        occ_orbitals[0], empty_orbitals[0], occ_energy, empty_energy, tau_points, partner, mirror,
        kpoints, columns, scale)
    return total.reshape(tau_points.shape[0], 1, -1, mirror.shape[0])


def shards(*args):
    kpoints, columns = lax.axis_size("kpt"), lax.axis_size("col")
    nrows, nocc, nemp = args[0].shape[1], args[0].shape[2], args[1].shape[2]
    times, window = args[4].shape[0], args[6].shape[0]
    slab, width = nrows // kpoints, nocc + nemp
    held = 2 * width * (kpoints * window + 4 * nrows + times * nrows) + 8 * times * nrows * window
    aligned = window % (2 * LANES) == 0 and nrows % LANES == 0 and nocc % LANES == 0 and nemp % LANES == 0
    aligned = aligned and (slab // columns) % 16 == 0 and slab % columns == 0 and nrows % kpoints == 0
    fits = aligned and held <= LINE_BYTES and kpoints & (kpoints - 1) == 0
    if lax.axis_size("row") == 2 and fits:
        return shards_line(*args)
    return shards_reduced(*args)


def solution(mesh):
    return jax.shard_map(
        shards,
        mesh=mesh,
        in_specs=(P("kpt", "row", None), P("kpt", "row", None), P(), P(), P(), P(), P("col")),
        out_specs=P(None, "row", "kpt", "col"),
        check_vma=False,
    )
```
